32 devices in a mesh: seq: 8 (over z, core), feat: 4 (over y, x).
Axes of the slice: x: 2, y: 2, z: 4, core: 2. Of those that a mesh axis runs over, the one named last changes fastest.
Arguments:
- activations: bfloat16 [2048, 6144], P('seq', 'feat'), may hold values from -15 to 15
- ridge_scale: float32 [], replicated, may hold values from 0.5 to 2
Outputs:
- whitened: bfloat16 [2048, 6144], P('seq', 'feat')
The draws below stay inside these ranges and needn't reach their ends.
All inputs are finite; a program needn't handle non-finite values.
Results may differ from the reference program's by a relative error of at most 0.0033.
Values sent between devices are 32-bit elements; how exact they have to be, the bound alone decides.
A program may use at most 128 MiB of HBM per device.

```python
import math
import jax
import jax.numpy as jnp
from jax import lax

D = 6144
RANK = 128
TOK_DEV = 256
ITERS = 1
ROOT_STEPS = 12
LEVELS = 3
TOKENS = 2048
N_SEQ = 8


def draw_activations(key, part):
    columns = jnp.exp(jax.random.uniform(jax.random.fold_in(key, 11), (D,), jnp.float32, math.log(0.3), math.log(3.0)))
    noise_rows = jnp.clip(jax.random.normal(jax.random.fold_in(key, 12), (TOKENS, D), jnp.float32), -5.0, 5.0)
    return (noise_rows * columns[None, :]).astype(jnp.bfloat16)


def setup_inputs(seed: int = 0) -> dict:
    streams_of = jax.random.split(jax.random.key(seed), 3)
    activations = draw_activations(jax.random.fold_in(streams_of[2], 71), 0)
    ridge_scale = jnp.clip(jnp.exp(jax.random.uniform(streams_of[1], (), jnp.float32, math.log(0.5), math.log(2.0))), 0.5, 2.0)
    return dict(activations=activations, ridge_scale=ridge_scale)


precise = lax.Precision.HIGHEST

def product(left_matrix, right_matrix):
    return jnp.dot(left_matrix, right_matrix, precision=precise)

def reduce_gram(stacked_gram):
    rank_size = stacked_gram.shape[0] // 2
    identity = jnp.eye(rank_size, dtype=stacked_gram.dtype)
    subspace = jnp.concatenate([identity, identity], axis=0) * 0.7071067811865476
    for repeat in range(ITERS):
        image_cols = product(stacked_gram, subspace)
        factor = jnp.linalg.cholesky(product(image_cols.T, image_cols))
        subspace = jax.scipy.linalg.solve_triangular(factor, image_cols.T, lower=True).T
    quotient = product(subspace.T, product(stacked_gram, subspace))
    quotient = 0.5 * (quotient + quotient.T)
    tail_mass = (jnp.trace(stacked_gram) - jnp.trace(quotient)) / rank_size
    root_factor = jnp.linalg.cholesky(quotient)
    inner_gram = product(root_factor.T, root_factor) + tail_mass * identity
    lower_factor = jnp.linalg.cholesky(inner_gram)
    return jax.scipy.linalg.solve_triangular(lower_factor, product(root_factor.T, subspace.T), lower=True)

def combine(earlier, later):
    own_gram = product(earlier, earlier.T)
    cross_gram = product(earlier, later.T)
    last_gram = product(later, later.T)
    stacked_gram = jnp.concatenate([jnp.concatenate([own_gram, cross_gram], 1), jnp.concatenate([cross_gram.T, last_gram], 1)], 0)
    mixing = reduce_gram(stacked_gram)
    return product(mixing, jnp.concatenate([earlier, later], 0))

def square_root(matrix):
    identity = jnp.eye(matrix.shape[0], dtype=matrix.dtype)
    norm_size = jnp.sqrt(jnp.sum(matrix * matrix))
    current = matrix / norm_size
    partner = identity
    for repeat in range(ROOT_STEPS):
        middle = 1.5 * identity - 0.5 * product(partner, current)
        current = product(current, middle)
        partner = product(middle, partner)
    return current * jnp.sqrt(norm_size)

def whiten(slab_rows, prefix, seen_rows, ridge_scale):
    scaled = prefix * lax.rsqrt(seen_rows * ridge_scale)
    small_gram = product(scaled, scaled.T)
    identity = jnp.eye(small_gram.shape[0], dtype=small_gram.dtype)
    shifted = identity + small_gram
    total_gram = shifted + square_root(shifted)
    total_gram = 0.5 * (total_gram + total_gram.T)
    half_basis = scaled.astype(jnp.bfloat16)
    projection = jnp.dot(slab_rows.astype(jnp.float32), half_basis.T.astype(jnp.float32), preferred_element_type=jnp.float32)
    coefficients = jax.scipy.linalg.cho_solve((jnp.linalg.cholesky(total_gram), True), projection.T).T
    restored = jnp.dot(coefficients.astype(jnp.bfloat16).astype(jnp.float32), half_basis.astype(jnp.float32), preferred_element_type=jnp.float32)
    return ((slab_rows.astype(jnp.float32) - restored) * lax.rsqrt(ridge_scale)).astype(jnp.bfloat16)

def reference(activations, ridge_scale):
    block_count = TOK_DEV // (2 * RANK)
    wide_rows = activations.reshape(N_SEQ * block_count, 2 * RANK, D).astype(jnp.float32)
    slab_grams = jnp.einsum('bik,bjk->bij', wide_rows, wide_rows, precision=precise)
    mixtures = jax.vmap(reduce_gram)(slab_grams)
    sketches = jnp.einsum('bij,bjk->bik', mixtures, wide_rows, precision=precise).reshape(N_SEQ, block_count, RANK, D)
    slab_sketch = sketches[:, 0]
    for block_index in range(1, block_count):
        slab_sketch = jax.vmap(combine)(slab_sketch, sketches[:, block_index])
    seq_index = jnp.arange(N_SEQ, dtype=jnp.int32)
    tree_block = slab_sketch
    prefix = slab_sketch
    for tree_level in range(LEVELS):
        sibling = jnp.bitwise_xor(seq_index, jnp.int32(1 << tree_level))
        partner = tree_block[sibling]
        merged = jax.vmap(combine)(partner, prefix)
        has_bit = seq_index // (1 << tree_level) % 2 == 1
        prefix = jnp.where(has_bit[:, None, None], merged, prefix)
        if tree_level + 1 < LEVELS:
            tree_block = jax.vmap(combine)(tree_block, partner)
    seen_rows = ((seq_index + 1) * TOK_DEV).astype(jnp.float32)
    slabs = activations.reshape(N_SEQ, TOK_DEV, D)
    whitened = jax.vmap(whiten, in_axes=(0, 0, 0, None))(slabs, prefix, seen_rows, ridge_scale)
    return whitened.reshape(N_SEQ * TOK_DEV, D)
```

```python
import functools

import jax
import jax.numpy as jnp
from jax import lax
from jax.experimental import pallas as pl
from jax.experimental.pallas import tpu as pltpu
from jax.sharding import PartitionSpec as P

RANK = 128
ROOT_STEPS = 12
PANEL = 16
MESH = pl.DeviceIdType.MESH
HIGHEST = lax.Precision.HIGHEST


def mm(a, b):
    return jnp.dot(a, b, precision=HIGHEST, preferred_element_type=jnp.float32)


def mm_t(a, b):
    return lax.dot_general(
        a, b, (((1,), (1,)), ((), ())), precision=HIGHEST, preferred_element_type=jnp.float32
    )


def split_3(x):
    high = x.astype(jnp.bfloat16)
    rest = x - high.astype(jnp.float32)
    middle = rest.astype(jnp.bfloat16)
    low = (rest - middle.astype(jnp.float32)).astype(jnp.bfloat16)
    return high, middle, low


def eye():
    rows = lax.broadcasted_iota(jnp.int32, (RANK, RANK), 0)
    columns = lax.broadcasted_iota(jnp.int32, (RANK, RANK), 1)
    return jnp.where(rows == columns, 1.0, 0.0).astype(jnp.float32)


def trace(matrix):
    size = matrix.shape[0]
    rows = lax.broadcasted_iota(jnp.int32, (size, size), 0)
    columns = lax.broadcasted_iota(jnp.int32, (size, size), 1)
    kept = jnp.where(rows == columns, matrix, 0.0)
    return jnp.sum(jnp.sum(kept, axis=1, keepdims=True), axis=0, keepdims=True)


def factorize(matrices, work):
    count = len(matrices)
    for k in range(count):
        work[k, :, :RANK] = matrices[k]
        work[k, :, RANK:] = eye()
    lane = lax.broadcasted_iota(jnp.int32, (PANEL, RANK), 1)
    sub = lax.broadcasted_iota(jnp.int32, (PANEL, RANK), 0)

    def step(index, carry):
        first = pl.multiple_of(index * PANEL, PANEL)
        left = [work[k, pl.ds(first, PANEL), :RANK] for k in range(count)]
        right = [work[k, pl.ds(first, PANEL), RANK:] for k in range(count)]
        columns = [
            [
                jnp.broadcast_to(
                    jnp.sum(jnp.where(lane == first + c, left[k], 0.0), axis=1, keepdims=True),
                    (PANEL, RANK),
                )
                for c in range(PANEL)
            ]
            for k in range(count)
        ]
        for i in range(PANEL):
            for k in range(count):
                scale = lax.rsqrt(columns[k][i][i : i + 1, :])
                factor = jnp.where(sub > i, columns[k][i], 0.0) * scale
                for c in range(i + 1, PANEL):
                    columns[k][c] -= factor * (columns[k][c][i : i + 1, :] * scale)
                row_left = left[k][i : i + 1, :] * scale
                row_right = right[k][i : i + 1, :] * scale
                left[k] = jnp.where(sub == i, row_left, left[k] - factor * row_left)
                right[k] = jnp.where(sub == i, row_right, right[k] - factor * row_right)
        for k in range(count):
            work[k, pl.ds(first, PANEL), :RANK] = left[k]
            work[k, pl.ds(first, PANEL), RANK:] = right[k]
            h, m, l = split_3(jnp.where(lane >= first + PANEL, left[k], 0.0))
            lh, lm, ll = split_3(left[k])
            rh, rm, rl = split_3(right[k])
            h, m, l = (part.astype(jnp.float32) for part in (h, m, l))
            lhs = jnp.concatenate([h, h, m, m, h, l, jnp.zeros((2 * PANEL, RANK), jnp.float32)], axis=0)
            lhs = lhs.T.astype(jnp.bfloat16)
            for part, (a, b, c) in enumerate([(lh, lm, ll), (rh, rm, rl)]):
                rhs = jnp.concatenate([a, b, a, b, c, a, jnp.zeros((2 * PANEL, RANK), jnp.bfloat16)], axis=0)
                work[k, :, part * RANK : (part + 1) * RANK] -= jnp.dot(
                    lhs, rhs, preferred_element_type=jnp.float32
                )
        return carry

    lax.fori_loop(0, RANK // PANEL, step, 0)
    rows = lax.broadcasted_iota(jnp.int32, (RANK, RANK), 0)
    cols = lax.broadcasted_iota(jnp.int32, (RANK, RANK), 1)
    return [
        (jnp.where(cols >= rows, work[k, :, :RANK], 0.0), work[k, :, RANK:]) for k in range(count)
    ]


def reduce_grams(grams, work):
    images = [(gram[:RANK, :] + gram[RANK:, :]) * 0.7071067811865476 for gram in grams]
    factors = factorize([mm_t(image, image) for image in images], work)
    bases = [mm(inverse, image) for (_, inverse), image in zip(factors, images)]
    quotients = [mm_t(mm(basis, gram), basis) for basis, gram in zip(bases, grams)]
    quotients = [0.5 * (quotient + quotient.T) for quotient in quotients]
    tails = [(trace(gram) - trace(quotient)) / RANK for gram, quotient in zip(grams, quotients)]
    uppers = [upper for upper, _ in factorize(quotients, work)]
    factors = factorize([mm_t(u, u) + tail * eye() for u, tail in zip(uppers, tails)], work)
    out = []
    for (_, inverse), upper, basis, gram in zip(factors, uppers, bases, grams):
        mixing = mm(mm(inverse, upper), basis)
        out.append((mixing, mm_t(mm(mixing, gram), mixing)))
    return out


def kernel(levels, feats, ridge_ref, rows_ref, out_ref, *scratch):
    work, tree, prefix, partner, grams, partner_grams = scratch[:6]
    slab_slots = scratch[6]
    level_slots = scratch[7 : 7 + levels]
    last_slots = scratch[7 + levels]
    send_sem, recv_sem, pair_send, pair_recv = scratch[8 + levels :]
    seq = lax.axis_index("seq")
    feat = lax.axis_index("feat")
    width = rows_ref.shape[1]

    def bit_of(level):
        return lax.rem(seq // (1 << level), 2)

    def sibling(level):
        return seq + (1 << level) - 2 * (1 << level) * bit_of(level)

    barrier = pltpu.get_barrier_semaphore()
    for offset in range(1, feats):
        pl.semaphore_signal(
            barrier, inc=1, device_id=(seq, lax.rem(feat + offset, feats)), device_id_type=MESH
        )
    for level in range(levels):
        pl.semaphore_signal(
            barrier, inc=1, device_id=(sibling(level), feat), device_id_type=MESH
        )
    pl.semaphore_wait(barrier, feats - 1 + levels)

    def send_sum(slots, phase):
        copies = []
        for offset in range(1, feats):
            copy = pltpu.make_async_remote_copy(
                src_ref=slots.at[feat],
                dst_ref=slots.at[feat],
                send_sem=send_sem.at[phase, offset],
                recv_sem=recv_sem.at[phase, offset],
                device_id=(seq, lax.rem(feat + offset, feats)),
                device_id_type=MESH,
            )
            copy.start()
            copies.append(copy)
        return copies

    def finish_sum(slots, copies):
        for copy in copies:
            copy.wait()
        total = slots[0]
        for index in range(1, feats):
            total = total + slots[index]
        return total

    rows = rows_ref[...]
    slab_slots[feat] = lax.dot_general(
        rows, rows, (((1,), (1,)), ((), ())), preferred_element_type=jnp.float32
    )
    gram = finish_sum(slab_slots, send_sum(slab_slots, 0))
    ((mixing, own_gram),) = reduce_grams([gram], work)
    h, m, l = split_3(mixing)
    sketch = (
        jnp.dot(l, rows, preferred_element_type=jnp.float32)
        + jnp.dot(m, rows, preferred_element_type=jnp.float32)
        + jnp.dot(h, rows, preferred_element_type=jnp.float32)
    )
    tree[0] = sketch
    prefix[...] = sketch
    grams[0] = own_gram
    prefix_gram = own_gram

    for level in range(levels):
        copies = []
        for index, (source, target) in enumerate(
            [(tree.at[level], partner.at[level]), (grams.at[level], partner_grams.at[level])]
        ):
            copy = pltpu.make_async_remote_copy(
                src_ref=source,
                dst_ref=target,
                send_sem=pair_send.at[level, index],
                recv_sem=pair_recv.at[level, index],
                device_id=(sibling(level), feat),
                device_id_type=MESH,
            )
            copy.start()
            copies.append(copy)
        for copy in copies:
            copy.wait()
        slots = level_slots[level]
        with_prefix = level > 0
        with_tree = level + 1 < levels or level == 0
        lefts = []
        if with_tree:
            lefts.append((tree.at[level], grams[level]))
        if with_prefix:
            lefts.append((prefix, prefix_gram))
        for index, (left, _) in enumerate(lefts):
            slots[feat, index * RANK : (index + 1) * RANK, :] = mm_t(
                left[...], partner[level]
            )
        crosses = finish_sum(slots, send_sum(slots, 1 + level))
        other = partner_grams[level]
        stacked = []
        for index, (_, left_gram) in enumerate(lefts):
            cross = crosses[index * RANK : (index + 1) * RANK]
            stacked.append(
                jnp.concatenate(
                    [
                        jnp.concatenate([left_gram, cross], 1),
                        jnp.concatenate([cross.T, other], 1),
                    ],
                    0,
                )
            )
        results = reduce_grams(stacked, work)
        merged = []
        for (left, _), (mixing, new_gram) in zip(lefts, results):
            merged.append(
                (mm(mixing[:, :RANK], left[...]) + mm(mixing[:, RANK:], partner[level]), new_gram)
            )
        keep = bit_of(level) == 1
        prefix[...] = jnp.where(keep, merged[-1][0], prefix[...])
        prefix_gram = jnp.where(keep, merged[-1][1], prefix_gram)
        if level + 1 < levels:
            tree[level + 1] = merged[0][0]
            grams[level + 1] = merged[0][1]

    ridge = ridge_ref[0, 0]
    seen_rows = ((seq + 1) * rows_ref.shape[0]).astype(jnp.float32)
    seen = jnp.full((1, 1), seen_rows * ridge, jnp.float32)
    half_basis = (prefix[...] * lax.rsqrt(seen)).astype(jnp.bfloat16)
    last_slots[feat] = lax.dot_general(
        rows, half_basis, (((1,), (1,)), ((), ())), preferred_element_type=jnp.float32
    )
    copies = send_sum(last_slots, 1 + levels)
    shifted = eye() + prefix_gram / seen
    norm = jnp.sqrt(
        jnp.sum(jnp.sum(shifted * shifted, axis=1, keepdims=True), axis=0, keepdims=True)
    )

    work[0, :, :RANK] = shifted / norm
    work[0, :, RANK:] = eye()

    def root_step(index, carry):
        current, other = work[0, :, :RANK], work[0, :, RANK:]
        middle = 1.5 * eye() - 0.5 * mm(other, current)
        work[0, :, :RANK] = mm(current, middle)
        work[0, :, RANK:] = mm(middle, other)
        return carry

    lax.fori_loop(0, ROOT_STEPS, root_step, 0)
    current = work[0, :, :RANK]
    total_gram = shifted + current * jnp.sqrt(norm)
    total_gram = 0.5 * (total_gram + total_gram.T)
    ((_, inverse),) = factorize([total_gram], work)
    projection = finish_sum(last_slots, copies)
    coefficients = mm(mm_t(projection, inverse), inverse).astype(jnp.bfloat16)
    restored = jnp.dot(coefficients, half_basis, preferred_element_type=jnp.float32)
    out_ref[...] = (
        (rows.astype(jnp.float32) - restored) * lax.rsqrt(jnp.full((1, 1), ridge, jnp.float32))
    ).astype(jnp.bfloat16)


def on_device(activations, ridge_scale):
    tokens, width = activations.shape
    feats = lax.axis_size("feat")
    levels = lax.axis_size("seq").bit_length() - 1
    wide = (RANK, width)
    square = (RANK, RANK)
    f32 = jnp.float32
    scratch = [
        pltpu.VMEM((2, RANK, 2 * RANK), f32),
        pltpu.VMEM((levels,) + wide, f32),
        pltpu.VMEM(wide, f32),
        pltpu.VMEM((levels,) + wide, f32),
        pltpu.VMEM((levels,) + square, f32),
        pltpu.VMEM((levels,) + square, f32),
        pltpu.VMEM((feats, tokens, tokens), f32),
    ]
    for level in range(levels):
        count = 2 if 0 < level < levels - 1 else 1
        scratch.append(pltpu.VMEM((feats, count * RANK, RANK), f32))
    scratch.append(pltpu.VMEM((feats, tokens, RANK), f32))
    scratch += [
        pltpu.SemaphoreType.DMA((levels + 2, feats)),
        pltpu.SemaphoreType.DMA((levels + 2, feats)),
        pltpu.SemaphoreType.DMA((levels, 2)),
        pltpu.SemaphoreType.DMA((levels, 2)),
    ]
    return pl.pallas_call(
        functools.partial(kernel, levels, feats),
        out_shape=jax.ShapeDtypeStruct(activations.shape, activations.dtype),
        in_specs=[
            pl.BlockSpec(memory_space=pltpu.SMEM),
            pl.BlockSpec(memory_space=pltpu.VMEM),
        ],
        out_specs=pl.BlockSpec(memory_space=pltpu.VMEM),
        scratch_shapes=scratch,
        compiler_params=pltpu.CompilerParams(
            collective_id=0, has_side_effects=True, vmem_limit_bytes=60 * 1024 * 1024
        ),
    )(ridge_scale.reshape(1, 1), activations)


def solution(mesh):
    placed = (P("seq", "feat"), P())
    return jax.shard_map(
        on_device, mesh=mesh, in_specs=placed, out_specs=P("seq", "feat"), check_vma=False
    )
```

```python
import functools

import jax
import jax.numpy as jnp
from jax import lax
from jax.experimental import pallas as pl
from jax.experimental.pallas import tpu as pltpu
from jax.sharding import PartitionSpec as P

RANK = 128
ROOT_STEPS = 12
PANEL = 16
MESH = pl.DeviceIdType.MESH
HIGHEST = lax.Precision.HIGHEST


def mm(a, b):
    return jnp.dot(a, b, precision=HIGHEST, preferred_element_type=jnp.float32)


def mm_t(a, b):
    return lax.dot_general(
        a, b, (((1,), (1,)), ((), ())), precision=HIGHEST, preferred_element_type=jnp.float32
    )


def split_3(x):
    high = x.astype(jnp.bfloat16)
    rest = x - high.astype(jnp.float32)
    middle = rest.astype(jnp.bfloat16)
    low = (rest - middle.astype(jnp.float32)).astype(jnp.bfloat16)
    return high, middle, low


def eye():
    rows = lax.broadcasted_iota(jnp.int32, (RANK, RANK), 0)
    columns = lax.broadcasted_iota(jnp.int32, (RANK, RANK), 1)
    return jnp.where(rows == columns, 1.0, 0.0).astype(jnp.float32)


def trace(matrix):
    size = matrix.shape[0]
    rows = lax.broadcasted_iota(jnp.int32, (size, size), 0)
    columns = lax.broadcasted_iota(jnp.int32, (size, size), 1)
    kept = jnp.where(rows == columns, matrix, 0.0)
    return jnp.sum(jnp.sum(kept, axis=1, keepdims=True), axis=0, keepdims=True)


def factorize(matrices, work, inverse=True):
    count = len(matrices)
    for k in range(count):
        work[k, :, :RANK] = matrices[k]
        if inverse:
            work[k, :, RANK:] = eye()
    lane = lax.broadcasted_iota(jnp.int32, (PANEL, RANK), 1)
    sub = lax.broadcasted_iota(jnp.int32, (PANEL, RANK), 0)

    def step(index, carry):
        first = pl.multiple_of(index * PANEL, PANEL)
        left = [work[k, pl.ds(first, PANEL), :RANK] for k in range(count)]
        right = [work[k, pl.ds(first, PANEL), RANK:] for k in range(count) if inverse]
        columns = [
            [
                jnp.broadcast_to(
                    jnp.sum(jnp.where(lane == first + c, left[k], 0.0), axis=1, keepdims=True),
                    (PANEL, RANK),
                )
                for c in range(PANEL)
            ]
            for k in range(count)
        ]
        for i in range(PANEL):
            for k in range(count):
                scale = lax.rsqrt(columns[k][i][i : i + 1, :])
                factor = jnp.where(sub > i, columns[k][i], 0.0) * scale
                for c in range(i + 1, PANEL):
                    columns[k][c] -= factor * (columns[k][c][i : i + 1, :] * scale)
                row_left = left[k][i : i + 1, :] * scale
                left[k] = jnp.where(sub == i, row_left, left[k] - factor * row_left)
                if inverse:
                    row_right = right[k][i : i + 1, :] * scale
                    right[k] = jnp.where(sub == i, row_right, right[k] - factor * row_right)
        for k in range(count):
            work[k, pl.ds(first, PANEL), :RANK] = left[k]
            if inverse:
                work[k, pl.ds(first, PANEL), RANK:] = right[k]
            h, m, l = split_3(jnp.where(lane >= first + PANEL, left[k], 0.0))
            sides = [split_3(side) for side in ([left[k], right[k]] if inverse else [left[k]])]
            h, m, l = (part.astype(jnp.float32) for part in (h, m, l))
            lhs = jnp.concatenate([h, h, m, m, h, l, jnp.zeros((2 * PANEL, RANK), jnp.float32)], axis=0)
            lhs = lhs.T.astype(jnp.bfloat16)
            for part, (a, b, c) in enumerate(sides):
                rhs = jnp.concatenate([a, b, a, b, c, a, jnp.zeros((2 * PANEL, RANK), jnp.bfloat16)], axis=0)
                work[k, :, part * RANK : (part + 1) * RANK] -= jnp.dot(
                    lhs, rhs, preferred_element_type=jnp.float32
                )
        return carry

    lax.fori_loop(0, RANK // PANEL, step, 0)
    rows = lax.broadcasted_iota(jnp.int32, (RANK, RANK), 0)
    cols = lax.broadcasted_iota(jnp.int32, (RANK, RANK), 1)
    return [
        (jnp.where(cols >= rows, work[k, :, :RANK], 0.0), work[k, :, RANK:] if inverse else None)
        for k in range(count)
    ]


def reduce_grams(grams, work):
    images = [(gram[:RANK, :] + gram[RANK:, :]) * 0.7071067811865476 for gram in grams]
    factors = factorize([mm_t(image, image) for image in images], work)
    bases = [mm(inverse, image) for (_, inverse), image in zip(factors, images)]
    quotients = [mm_t(mm(basis, gram), basis) for basis, gram in zip(bases, grams)]
    quotients = [0.5 * (quotient + quotient.T) for quotient in quotients]
    tails = [(trace(gram) - trace(quotient)) / RANK for gram, quotient in zip(grams, quotients)]
    uppers = [upper for upper, _ in factorize(quotients, work, False)]
    factors = factorize([mm_t(u, u) + tail * eye() for u, tail in zip(uppers, tails)], work)
    out = []
    for (_, inverse), upper, basis, gram in zip(factors, uppers, bases, grams):
        mixing = mm(mm(inverse, upper), basis)
        out.append((mixing, mm_t(mm(mixing, gram), mixing)))
    return out


def kernel(levels, feats, ridge_ref, rows_ref, out_ref, *scratch):
    work, tree, prefix, partner = scratch[:4]
    slab_slots = scratch[4]
    level_slots = scratch[5 : 5 + levels]
    last_slots = scratch[5 + levels]
    send_sem, recv_sem, pair_send, pair_recv = scratch[6 + levels :]
    seq = lax.axis_index("seq")
    feat = lax.axis_index("feat")
    width = rows_ref.shape[1]

    def bit_of(level):
        return lax.rem(seq // (1 << level), 2)

    def sibling(level):
        return seq + (1 << level) - 2 * (1 << level) * bit_of(level)

    barrier = pltpu.get_barrier_semaphore()
    for offset in range(1, feats):
        pl.semaphore_signal(
            barrier, inc=1, device_id=(seq, lax.rem(feat + offset, feats)), device_id_type=MESH
        )
    for level in range(levels):
        pl.semaphore_signal(
            barrier, inc=1, device_id=(sibling(level), feat), device_id_type=MESH
        )
    pl.semaphore_wait(barrier, feats - 1 + levels)

    def send_sum(slots, phase):
        copies = []
        for offset in range(1, feats):
            copy = pltpu.make_async_remote_copy(
                src_ref=slots.at[feat],
                dst_ref=slots.at[feat],
                send_sem=send_sem.at[phase, offset],
                recv_sem=recv_sem.at[phase, offset],
                device_id=(seq, lax.rem(feat + offset, feats)),
                device_id_type=MESH,
            )
            copy.start()
            copies.append(copy)
        return copies

    def finish_sum(slots, copies):
        for copy in copies:
            copy.wait()
        total = slots[0]
        for index in range(1, feats):
            total = total + slots[index]
        return total

    def fetch(level):
        for index, hop in enumerate(range(level, -1, -1)):
            source = tree if hop == level else partner
            bits = hop if hop == level else hop + 1
            size = RANK >> bits
            first = 0
            for bit in range(bits):
                first = first + bit_of(bit) * (RANK >> (bit + 1))
            span = pl.ds(pl.multiple_of(first, size), size) if bits else pl.ds(0, RANK)
            copy = pltpu.make_async_remote_copy(
                src_ref=source.at[level, span],
                dst_ref=partner.at[level, span],
                send_sem=pair_send.at[level, index],
                recv_sem=pair_recv.at[level, index],
                device_id=(sibling(hop), feat),
                device_id_type=MESH,
            )
            copy.start()
            copy.wait()

    rows = rows_ref[...]
    slab_slots[feat] = lax.dot_general(
        rows, rows, (((1,), (1,)), ((), ())), preferred_element_type=jnp.float32
    )
    gram = finish_sum(slab_slots, send_sum(slab_slots, 0))
    ((mixing, own_gram),) = reduce_grams([gram], work)
    h, m, l = split_3(mixing)
    sketch = (
        jnp.dot(l, rows, preferred_element_type=jnp.float32)
        + jnp.dot(m, rows, preferred_element_type=jnp.float32)
        + jnp.dot(h, rows, preferred_element_type=jnp.float32)
    )
    tree[0, :, :width] = sketch
    tree[0, :, width:] = own_gram
    prefix[...] = sketch
    prefix_gram = own_gram

    for level in range(levels):
        fetch(level)
        slots = level_slots[level]
        with_prefix = level > 0
        with_tree = level + 1 < levels or level == 0
        lefts = []
        if with_tree:
            lefts.append((tree.at[level, :, :width], tree[level, :, width:]))
        if with_prefix:
            lefts.append((prefix, prefix_gram))
        for index, (left, _) in enumerate(lefts):
            slots[feat, index * RANK : (index + 1) * RANK, :] = mm_t(
                left[...], partner[level, :, :width]
            )
        crosses = finish_sum(slots, send_sum(slots, 1 + level))
        other = partner[level, :, width:]
        stacked = []
        for index, (_, left_gram) in enumerate(lefts):
            cross = crosses[index * RANK : (index + 1) * RANK]
            stacked.append(
                jnp.concatenate(
                    [
                        jnp.concatenate([left_gram, cross], 1),
                        jnp.concatenate([cross.T, other], 1),
                    ],
                    0,
                )
            )
        results = reduce_grams(stacked, work)
        merged = []
        for (left, _), (mixing, new_gram) in zip(lefts, results):
            merged.append(
                (mm(mixing[:, :RANK], left[...]) + mm(mixing[:, RANK:], partner[level, :, :width]), new_gram)
            )
        keep = bit_of(level) == 1
        prefix[...] = jnp.where(keep, merged[-1][0], prefix[...])
        prefix_gram = jnp.where(keep, merged[-1][1], prefix_gram)
        if level + 1 < levels:
            tree[level + 1, :, :width] = merged[0][0]
            tree[level + 1, :, width:] = merged[0][1]

    ridge = ridge_ref[0, 0]
    seen_rows = ((seq + 1) * rows_ref.shape[0]).astype(jnp.float32)
    seen = jnp.full((1, 1), seen_rows * ridge, jnp.float32)
    half_basis = (prefix[...] * lax.rsqrt(seen)).astype(jnp.bfloat16)
    last_slots[feat] = lax.dot_general(
        rows, half_basis, (((1,), (1,)), ((), ())), preferred_element_type=jnp.float32
    )
    copies = send_sum(last_slots, 1 + levels)
    shifted = eye() + prefix_gram / seen
    norm = jnp.sqrt(
        jnp.sum(jnp.sum(shifted * shifted, axis=1, keepdims=True), axis=0, keepdims=True)
    )

    work[0, :, :RANK] = shifted / norm
    work[0, :, RANK:] = eye()

    def root_step(index, carry):
        current, other = work[0, :, :RANK], work[0, :, RANK:]
        middle = 1.5 * eye() - 0.5 * mm(other, current)
        work[0, :, :RANK] = mm(current, middle)
        work[0, :, RANK:] = mm(middle, other)
        return carry

    lax.fori_loop(0, ROOT_STEPS, root_step, 0)
    current = work[0, :, :RANK]
    total_gram = shifted + current * jnp.sqrt(norm)
    total_gram = 0.5 * (total_gram + total_gram.T)
    ((_, inverse),) = factorize([total_gram], work)
    projection = finish_sum(last_slots, copies)
    coefficients = mm(mm_t(projection, inverse), inverse).astype(jnp.bfloat16)
    restored = jnp.dot(coefficients, half_basis, preferred_element_type=jnp.float32)
    out_ref[...] = (
        (rows.astype(jnp.float32) - restored) * lax.rsqrt(jnp.full((1, 1), ridge, jnp.float32))
    ).astype(jnp.bfloat16)


def on_device(activations, ridge_scale):
    tokens, width = activations.shape
    feats = lax.axis_size("feat")
    levels = lax.axis_size("seq").bit_length() - 1
    wide = (RANK, width)
    f32 = jnp.float32
    scratch = [
        pltpu.VMEM((2, RANK, 2 * RANK), f32),
        pltpu.VMEM((levels, RANK, width + RANK), f32),
        pltpu.VMEM(wide, f32),
        pltpu.VMEM((levels, RANK, width + RANK), f32),
        pltpu.VMEM((feats, tokens, tokens), f32),
    ]
    for level in range(levels):
        count = 2 if 0 < level < levels - 1 else 1
        scratch.append(pltpu.VMEM((feats, count * RANK, RANK), f32))
    scratch.append(pltpu.VMEM((feats, tokens, RANK), f32))
    scratch += [
        pltpu.SemaphoreType.DMA((levels + 2, feats)),
        pltpu.SemaphoreType.DMA((levels + 2, feats)),
        pltpu.SemaphoreType.DMA((levels, levels)),
        pltpu.SemaphoreType.DMA((levels, levels)),
    ]
    return pl.pallas_call(
        functools.partial(kernel, levels, feats),
        out_shape=jax.ShapeDtypeStruct(activations.shape, activations.dtype),
        in_specs=[
            pl.BlockSpec(memory_space=pltpu.SMEM),
            pl.BlockSpec(memory_space=pltpu.VMEM),
        ],
        out_specs=pl.BlockSpec(memory_space=pltpu.VMEM),
        scratch_shapes=scratch,
        compiler_params=pltpu.CompilerParams(
            collective_id=0, has_side_effects=True, vmem_limit_bytes=60 * 1024 * 1024
        ),
    )(ridge_scale.reshape(1, 1), activations)


def solution(mesh):
    placed = (P("seq", "feat"), P())
    return jax.shard_map(
        on_device, mesh=mesh, in_specs=placed, out_specs=P("seq", "feat"), check_vma=False
    )
```
